32 devices in a mesh: replica: 4 (over z), data: 8 (over y, x, core).
Axes of the slice: x: 2, y: 2, z: 4, core: 2. Of those that a mesh axis runs over, the one named last changes fastest.
Arguments:
- hidden_in: bfloat16 [512, 32, 1280], P(('replica', 'data'))
- grad_out: bfloat16 [512, 32, 1280], P(('replica', 'data'))
- gain_attn: float32 [3, 1280], replicated
- gain_mlp: float32 [3, 1280], replicated
- w_qkv: bfloat16 [3, 1280, 3, 20, 64], replicated
- w_out: bfloat16 [3, 20, 64, 1280], replicated
- w_up: bfloat16 [3, 1280, 5120], replicated
- w_down: bfloat16 [3, 5120, 1280], replicated
Outputs:
- output 1: bfloat16 [512, 32, 1280], P(('replica', 'data'))
- output 2: float32 [3, 19663360], P(None, 'data')
All inputs are finite; a program needn't handle non-finite values.
Results may differ from the reference program's by a relative error of at most 0.02.
Values are sent between devices in bfloat16 or wider.
A program may use at most 1 GiB of HBM per device.

```python
import jax
import jax.numpy as jnp
from jax import lax

WIDTH = 1280
FFN = 5120
HEADS = 20
LAYERS = 3
BATCH_DEV = 16
SEQ = 32
SHARDS = 32

HEAD_DIM = WIDTH // HEADS
BATCH = BATCH_DEV * SHARDS
LAYER_PARAMS = 2 * WIDTH + 4 * WIDTH * WIDTH + 2 * WIDTH * FFN
RMS_EPS = 1e-5
MASK_FILL = -1e30


def setup_inputs(seed: int = 0) -> dict:
    rng_keys = jax.random.split(jax.random.key(seed), 8)
    hidden_in = jax.random.normal(rng_keys[0], (BATCH, SEQ, WIDTH), jnp.float32)
    grad_out = jax.random.normal(rng_keys[1], (BATCH, SEQ, WIDTH), jnp.float32)
    gain_attn = 1.0 + 0.3 * jax.random.normal(rng_keys[2], (LAYERS, WIDTH), jnp.float32)
    gain_mlp = 1.0 + 0.3 * jax.random.normal(rng_keys[3], (LAYERS, WIDTH), jnp.float32)
    w_qkv = jax.random.normal(rng_keys[4], (LAYERS, WIDTH, 3, HEADS, HEAD_DIM), jnp.float32) * WIDTH ** -0.5
    w_out = jax.random.normal(rng_keys[5], (LAYERS, HEADS, HEAD_DIM, WIDTH), jnp.float32) * WIDTH ** -0.5
    w_up = jax.random.normal(rng_keys[6], (LAYERS, WIDTH, FFN), jnp.float32) * WIDTH ** -0.5
    w_down = jax.random.normal(rng_keys[7], (LAYERS, FFN, WIDTH), jnp.float32) * FFN ** -0.5
    return {
        "hidden_in": hidden_in.astype(jnp.bfloat16),
        "grad_out": grad_out.astype(jnp.bfloat16),
        "gain_attn": gain_attn,
        "gain_mlp": gain_mlp,
        "w_qkv": w_qkv.astype(jnp.bfloat16),
        "w_out": w_out.astype(jnp.bfloat16),
        "w_up": w_up.astype(jnp.bfloat16),
        "w_down": w_down.astype(jnp.bfloat16),
    }


def rms_scale(act_in, gain_vec):
    act32 = act_in.astype(jnp.float32)
    inv_rms = lax.rsqrt(jnp.mean(act32 * act32, axis=-1, keepdims=True) + RMS_EPS)
    return (act32 * inv_rms * gain_vec).astype(jnp.bfloat16)


def mm_round(eq_form, lhs_arr, rhs_arr):
    return jnp.einsum(eq_form, lhs_arr.astype(jnp.float32), rhs_arr.astype(jnp.float32)).astype(jnp.bfloat16)


def add_round(lhs_arr, rhs_arr):
    return (lhs_arr.astype(jnp.float32) + rhs_arr.astype(jnp.float32)).astype(jnp.bfloat16)


def causal_attention(queries, keys_in, values):
    seq_len = queries.shape[1]
    scores = jnp.einsum("bqhe,bkhe->bhqk", queries.astype(jnp.float32), keys_in.astype(jnp.float32)) * queries.shape[-1] ** -0.5
    causal = jnp.arange(seq_len)[:, None] >= jnp.arange(seq_len)[None, :]
    scores = jnp.where(causal, scores, MASK_FILL)
    attn_probs = jax.nn.softmax(scores, axis=-1).astype(jnp.bfloat16)
    return mm_round("bhqk,bkhe->bqhe", attn_probs, values)


def layer_forward(act_in, layer_params):
    gain_a, gain_m, wqkv_l, wout_l, wup_l, wdown_l = layer_params
    normed_a = rms_scale(act_in, gain_a)
    qkv_proj = mm_round("bsd,dthe->bsthe", normed_a, wqkv_l)
    context = causal_attention(qkv_proj[:, :, 0], qkv_proj[:, :, 1], qkv_proj[:, :, 2])
    hidden = add_round(act_in, mm_round("bshe,hed->bsd", context, wout_l))
    normed_m = rms_scale(hidden, gain_m)
    gelu_out = jax.nn.gelu(mm_round("bsd,df->bsf", normed_m, wup_l).astype(jnp.float32)).astype(jnp.bfloat16)
    block_out = add_round(hidden, mm_round("bsf,fd->bsd", gelu_out, wdown_l))
    return block_out, None


def stack_forward(act_in, params):
    return lax.scan(layer_forward, act_in, params)[0]


def flat_layer_grads(layer_grads):
    return jnp.concatenate([piece.astype(jnp.bfloat16).reshape(LAYERS, -1) for piece in layer_grads], axis=1)


def reference(hidden_in, grad_out, gain_attn, gain_mlp, w_qkv, w_out, w_up, w_down):
    params = (gain_attn, gain_mlp, w_qkv, w_out, w_up, w_down)
    in_shards = hidden_in.reshape(SHARDS, BATCH_DEV, SEQ, WIDTH)
    cot_shards = grad_out.reshape(SHARDS, BATCH_DEV, SEQ, WIDTH)

    def shard_step(grad_sum, shard_pair):
        act_loc, cot_loc = shard_pair
        _, pullback = jax.vjp(stack_forward, act_loc, params)
        d_act, d_params = pullback(cot_loc)
        return grad_sum + flat_layer_grads(d_params).astype(jnp.float32), d_act

    init_sum = jnp.zeros((LAYERS, LAYER_PARAMS), jnp.float32)
    grad_sum, d_shards = lax.scan(shard_step, init_sum, (in_shards, cot_shards))
    return d_shards.reshape(BATCH, SEQ, WIDTH), grad_sum / SHARDS
```

```python
import functools

import jax
import jax.numpy as jnp
from jax import lax
from jax.experimental import pallas as pl
from jax.experimental.pallas import tpu as pltpu
from jax.sharding import PartitionSpec as P

RMS_EPS = 1e-5
MASK_FILL = -1e30
CHUNKS = 4
INTERPRET = False


def rms_scale(act_in, gain_vec):
    act32 = act_in.astype(jnp.float32)
    inv_rms = lax.rsqrt(jnp.mean(act32 * act32, axis=-1, keepdims=True) + RMS_EPS)
    return (act32 * inv_rms * gain_vec).astype(jnp.bfloat16)


def gelu_round(up_proj):
    return jax.nn.gelu(up_proj.astype(jnp.float32)).astype(jnp.bfloat16)


def mm_round(eq_form, lhs_arr, rhs_arr):
    return jnp.einsum(eq_form, lhs_arr, rhs_arr, preferred_element_type=jnp.float32).astype(jnp.bfloat16)


def add_round(lhs_arr, rhs_arr):
    return (lhs_arr.astype(jnp.float32) + rhs_arr.astype(jnp.float32)).astype(jnp.bfloat16)


def causal_attention(queries, keys_in, values):
    seq_len = queries.shape[1]
    scores = jnp.einsum("bqhe,bkhe->bhqk", queries, keys_in, preferred_element_type=jnp.float32) * queries.shape[-1] ** -0.5
    causal = jnp.arange(seq_len)[:, None] >= jnp.arange(seq_len)[None, :]
    scores = jnp.where(causal, scores, MASK_FILL)
    attn_probs = jax.nn.softmax(scores, axis=-1).astype(jnp.bfloat16)
    return mm_round("bhqk,bkhe->bqhe", attn_probs, values)


def pick_tile(total, limit):
    best = 128
    for cand in range(128, min(total, limit) + 1, 128):
        if total % cand == 0:
            best = cand
    return best


def dw_kernel(tile_m, n_cols, chunk_n, base_unit, n_steps, gain_units, x_ref, dy_ref, *rest):
    if gain_units:
        gains_ref, _, flat_ref, acc_scr, out_scr, sem, gain_sem = rest
    else:
        flat_ref, acc_scr, out_scr, sem = rest[-4:]
        gains_ref = gain_sem = None
    step = pl.program_id(0)
    per_row = n_cols // 128
    units = tile_m * per_row // 16
    slot = lax.rem(step, 2)

    def out_copy(slot_idx, step_idx):
        return pltpu.make_async_copy(out_scr.at[slot_idx], flat_ref.at[pl.ds(base_unit + step_idx * units, units)], sem.at[slot_idx])

    if gain_units:
        @pl.when(step == 0)
        def _():
            pltpu.make_async_copy(gains_ref, flat_ref.at[pl.ds(0, gain_units)], gain_sem).start()

    @pl.when(step >= 2)
    def _():
        out_copy(slot, step - 2).wait()

    x_blk = x_ref[...]

    def body(idx, carry):
        col = pl.multiple_of(idx * chunk_n, chunk_n)
        acc = lax.dot_general(x_blk, dy_ref[:, pl.ds(col, chunk_n)], (((0,), (0,)), ((), ())), preferred_element_type=jnp.float32)
        for sub in range(chunk_n // 128):
            acc_scr[pl.ds(idx * (chunk_n // 128) + sub, tile_m, stride=per_row), :] = acc[:, sub * 128:(sub + 1) * 128]
        return carry

    lax.fori_loop(0, n_cols // chunk_n, body, 0)
    out_scr[slot] = acc_scr[...].astype(jnp.bfloat16).reshape(units, 16, 128)
    out_copy(slot, step).start()

    @pl.when(step == n_steps - 1)
    def _():
        if n_steps >= 2:
            out_copy(lax.rem(step + 1, 2), step - 1).wait()
        out_copy(slot, step).wait()
        if gain_units:
            pltpu.make_async_copy(gains_ref, flat_ref.at[pl.ds(0, gain_units)], gain_sem).wait()


def dw_flat(x_act, d_out, base_unit, total_units, flat=None, gains=None):
    tokens, m_rows = x_act.shape
    n_cols = d_out.shape[1]
    tile_m = pick_tile(m_rows, max(128, 6553600 // 5 // n_cols))
    chunk_n = pick_tile(n_cols, 640)
    n_steps = m_rows // tile_m
    units = tile_m * (n_cols // 128) // 16
    gain_units = gains.shape[0] if gains is not None else 0
    in_specs = [pl.BlockSpec((tokens, tile_m), lambda i: (0, i)), pl.BlockSpec((tokens, n_cols), lambda i: (0, 0))]
    args = [x_act, d_out]
    scratch = [pltpu.VMEM((tile_m * n_cols // 128, 128), jnp.float32), pltpu.VMEM((2, units, 16, 128), jnp.bfloat16), pltpu.SemaphoreType.DMA((2,))]
    if gains is not None:
        in_specs.append(pl.BlockSpec(gains.shape, lambda i: (0, 0, 0)))
        args.append(gains)
        scratch.append(pltpu.SemaphoreType.DMA(()))
    aliases = {}
    if flat is not None:
        in_specs.append(pl.BlockSpec(memory_space=pl.ANY))
        args.append(flat)
        aliases = {len(args) - 1: 0}
    return pl.pallas_call(
        functools.partial(dw_kernel, tile_m, n_cols, chunk_n, base_unit, n_steps, gain_units),
        out_shape=jax.ShapeDtypeStruct((total_units, 16, 128), jnp.bfloat16),
        grid=(n_steps,),
        in_specs=in_specs,
        out_specs=pl.BlockSpec(memory_space=pl.ANY),
        scratch_shapes=scratch,
        input_output_aliases=aliases,
        compiler_params=pltpu.CompilerParams(dimension_semantics=("arbitrary",), vmem_limit_bytes=48 * 1024 * 1024),
        cost_estimate=pl.CostEstimate(flops=2 * tokens * m_rows * n_cols, bytes_accessed=2 * (tokens * (m_rows + n_cols) + m_rows * n_cols), transcendentals=0),
        interpret=INTERPRET,
        name="dw_flat",
    )(*args)


def place_kernel(layers, blk, tail, head, half_rows, cur_ref, nxt_ref, out_ref, win_scr, mix_scr):
    dev = lax.axis_index("data")
    halves = 2 * head + half_rows * dev
    first = halves // 2
    odd = lax.rem(halves, 2) == 1
    low_lanes = lax.broadcasted_iota(jnp.int32, (8, 128), 1) < 64
    for layer in range(layers):
        win_scr[layer, pl.ds(0, blk), :] = cur_ref[layer]
        win_scr[layer, pl.ds(blk, tail), :] = nxt_ref[layer]

    def rows(idx, carry):
        base = pl.multiple_of(idx * 8, 8)
        for layer in range(layers):
            here = win_scr[layer, pl.ds(first + base, 8), :]
            after = win_scr[layer, pl.ds(first + base + 1, 8), :]
            shifted = jnp.where(low_lanes, pltpu.roll(here, 64, 1), pltpu.roll(after, 64, 1))
            mix_scr[pl.ds(4 * base + layer, 8, stride=4), :] = jnp.where(odd, shifted, here)
        for sub in range(8):
            lane = pl.multiple_of((base + sub) * 128, 128)
            out_ref[:, pl.ds(lane, 128)] = mix_scr[pl.ds(4 * (base + sub), 4), :][:layers]
        return carry

    lax.fori_loop(0, blk // 8, rows, 0)


def place_output(windows, share, blk, tail, head, half_rows):
    layers, n_rows, _ = windows.shape
    steps = -(-share // (128 * blk))
    last_tail = n_rows // tail - 1
    return pl.pallas_call(
        functools.partial(place_kernel, layers, blk, tail, head, half_rows),
        out_shape=jax.ShapeDtypeStruct((layers, share), jnp.float32),
        grid=(steps,),
        in_specs=[
            pl.BlockSpec((layers, blk, 128), lambda i: (0, i, 0)),
            pl.BlockSpec((layers, tail, 128), lambda i: (0, jnp.minimum((i + 1) * (blk // tail), last_tail), 0)),
        ],
        out_specs=pl.BlockSpec((layers, blk * 128), lambda i: (0, i)),
        scratch_shapes=[pltpu.VMEM((layers, blk + tail, 128), jnp.float32), pltpu.VMEM((blk * 4, 128), jnp.float32)],
        compiler_params=pltpu.CompilerParams(dimension_semantics=("arbitrary",), vmem_limit_bytes=48 * 1024 * 1024),
        cost_estimate=pl.CostEstimate(flops=100 * layers * share, bytes_accessed=8 * layers * share, transcendentals=0),
        interpret=INTERPRET,
        name="place_output",
    )(windows, windows)


def block_forward(act_in, gain_a, gain_m, w_qkv, w_out, w_up, w_down, total_units):
    n_seq, seq_len, width = act_in.shape
    tokens = n_seq * seq_len
    normed_a, norm_a_back = jax.vjp(rms_scale, act_in, gain_a)
    qkv_proj = mm_round("bsd,dthe->bsthe", normed_a, w_qkv)
    context, attn_back = jax.vjp(causal_attention, qkv_proj[:, :, 0], qkv_proj[:, :, 1], qkv_proj[:, :, 2])
    hidden = add_round(act_in, mm_round("bshe,hed->bsd", context, w_out))
    normed_m, norm_m_back = jax.vjp(rms_scale, hidden, gain_m)
    up_proj = mm_round("bsd,df->bsf", normed_m, w_up)
    gelu_out, gelu_back = jax.vjp(gelu_round, up_proj)
    block_out = add_round(hidden, mm_round("bsf,fd->bsd", gelu_out, w_down))

    def flat2(arr):
        return arr.reshape(tokens, -1)

    unit = 16 * 128
    at_qkv = CHUNKS
    at_out = at_qkv + w_qkv.size // unit
    at_up = at_out + w_out.size // unit
    at_down = at_up + w_up.size // unit

    def block_backward(d_out, order):
        (d_out,) = order.tie(d_out)
        flat = dw_flat(flat2(gelu_out), flat2(d_out), at_down, total_units)
        d_gelu = mm_round("bsd,fd->bsf", d_out, w_down)
        (d_up,) = gelu_back(d_gelu)
        order.mark(flat, d_up)
        yield None
        (d_up,) = order.tie(d_up)
        flat = dw_flat(flat2(normed_m), flat2(d_up), at_up, total_units, flat)
        d_normed_m = mm_round("bsf,df->bsd", d_up, w_up)
        order.mark(flat, d_normed_m)
        yield None
        (d_normed_m,) = order.tie(d_normed_m)
        d_hid_norm, d_gain_m = norm_m_back(d_normed_m)
        d_hidden = add_round(d_out, d_hid_norm)
        flat = dw_flat(flat2(context), flat2(d_hidden), at_out, total_units, flat)
        d_context = mm_round("bsd,hed->bshe", d_hidden, w_out)
        d_query, d_key, d_value = attn_back(d_context)
        d_qkv = jnp.stack([d_query, d_key, d_value], axis=2)
        order.mark(flat, d_qkv)
        yield None
        (d_qkv,) = order.tie(d_qkv)
        d_normed_a = mm_round("bsthe,dthe->bsd", d_qkv, w_qkv)
        d_act_norm, d_gain_a = norm_a_back(d_normed_a)
        d_act = add_round(d_hidden, d_act_norm)
        pad = jnp.zeros((CHUNKS * unit - 2 * width,), jnp.bfloat16)
        gains = jnp.concatenate([pad, d_gain_a.astype(jnp.bfloat16), d_gain_m.astype(jnp.bfloat16)]).reshape(CHUNKS, 16, 128)
        flat = dw_flat(flat2(normed_a), flat2(d_qkv), at_qkv, total_units, flat, gains)
        order.mark(flat, d_act)
        yield d_act, flat

    return block_out, block_backward


def add32(*parts):
    total = parts[0].astype(jnp.float32)
    for part in parts[1:]:
        total = (total + part.astype(jnp.float32)).astype(jnp.bfloat16).astype(jnp.float32)
    return total.astype(jnp.bfloat16)


class Order:
    def __init__(self):
        self.last = ()

    def tie(self, *arrays):
        return lax.optimization_barrier(arrays + self.last)[:len(arrays)]

    def mark(self, *arrays):
        self.last = arrays


class Chunk:
    def __init__(self, order, flat, chunk_idx, chunk_units, share_units, total_dev):
        self.order, self.flat, self.chunk_idx = order, flat, chunk_idx
        self.chunk_units, self.share_units, self.total_dev = chunk_units, share_units, total_dev
        dev = lax.axis_index("data")
        self.core, chip = lax.rem(dev, 2), dev // 2
        self.bits = (1, 2) if chunk_idx % 2 == 0 else (2, 1)
        self.chips = [chip, chip ^ self.bits[1], chip ^ self.bits[0], chip ^ 3]

    def piece(self, flat, pos, core_idx):
        start = (2 * self.chips[pos] + core_idx) * self.share_units + self.chunk_idx * self.chunk_units
        return lax.dynamic_slice_in_dim(flat, start, self.chunk_units, 0)

    def hop(self, value, bit):
        return lax.ppermute(value, "data", [(idx, idx ^ bit) for idx in range(8)])

    def core_hop(self):
        (flat,) = self.order.tie(self.flat)
        send = jnp.stack([self.piece(flat, pos, 1 - self.core) for pos in range(4)])
        self.order.mark(send)
        self.got_a = self.hop(send, 1)

    def first_hop(self):
        (got_a,) = self.order.tie(self.got_a)
        send = jnp.stack([add32(self.piece(self.flat, pos, self.core), got_a[pos]) for pos in (2, 3)])
        self.order.mark(send)
        self.got_b = self.hop(send, 2 * self.bits[0])

    def second_hop(self):
        (got_b,) = self.order.tie(self.got_b)
        send = add32(self.piece(self.flat, 1, self.core), self.got_a[1], got_b[1])
        self.order.mark(send)
        self.got_c = self.hop(send, 2 * self.bits[1])

    def z_in(self):
        (got_c,) = self.order.tie(self.got_c)
        self.mine = add32(self.piece(self.flat, 0, self.core), self.got_a[0], self.got_b[0], got_c)
        self.order.mark(self.mine)
        self.got_d = lax.ppermute(self.mine, "replica", [(0, 1), (3, 2)])

    def z_mid(self):
        (got_d,) = self.order.tie(self.got_d)
        self.pair = self.mine.astype(jnp.float32) + got_d.astype(jnp.float32)
        self.order.mark(self.pair)
        self.got_e = lax.ppermute(self.pair, "replica", [(1, 2), (2, 1)])

    def z_out(self):
        (got_e,) = self.order.tie(self.got_e)
        self.total = (self.pair + got_e) / self.total_dev
        self.order.mark(self.total)
        self.got_f = lax.ppermute(self.total, "replica", [(1, 0), (2, 3)])

    def finish(self, windows, layer):
        (got_f,) = self.order.tie(self.got_f)
        rep = lax.axis_index("replica")
        part = jnp.where((rep == 1) | (rep == 2), self.total, got_f)
        windows = lax.dynamic_update_slice(windows, part[None], (layer, self.chunk_idx * self.chunk_units, 0, 0))
        self.order.mark(windows)
        return windows


def run_plan(layers, make_segments, make_chunk, windows, order):
    pairs = layers * CHUNKS // 2
    chunks, finished = {}, []
    compute = []
    for layer in reversed(range(layers)):
        compute += [layer] * 4
    segments, flats = {}, {}
    state = {"windows": windows, "grad_act": None}

    def segment():
        if not compute:
            return
        layer = compute.pop(0)
        if layer not in segments:
            segments[layer] = make_segments(layer, state["grad_act"])
        out = next(segments[layer])
        if out is not None:
            state["grad_act"], flats[layer] = out

    def need(layer):
        while layer not in flats:
            segment()

    def each(pair, name):
        if pair < pairs:
            for idx in (2 * pair, 2 * pair + 1):
                getattr(chunks[idx], name)()

    def begin(pair):
        if pair < pairs:
            for idx in (2 * pair, 2 * pair + 1):
                layer = layers - 1 - idx // CHUNKS
                need(layer)
                chunks[idx] = make_chunk(flats[layer], idx % CHUNKS)
                chunks[idx].core_hop()
            each(pair, "first_hop")

    def finish(idx):
        if idx >= 0:
            state["windows"] = chunks[idx].finish(state["windows"], layers - 1 - idx // CHUNKS)

    begin(0)
    segment()
    segment()
    each(0, "second_hop")
    begin(1)
    segment()
    each(0, "z_in")
    segment()
    for pair in range(pairs):
        chunks[2 * pair].z_mid()
        if pair:
            chunks[2 * pair - 1].z_out()
        each(pair + 1, "second_hop")
        begin(pair + 2)
        finish(2 * pair - 3)
        segment()
        chunks[2 * pair + 1].z_mid()
        chunks[2 * pair].z_out()
        each(pair + 1, "z_in")
        finish(2 * pair - 2)
        segment()
    last = 2 * pairs - 1
    chunks[last].z_out()
    for idx in range(last - 2, last + 1):
        finish(idx)
    return state["grad_act"], state["windows"]


def solution(mesh):
    total_dev = mesh.shape["replica"] * mesh.shape["data"]
    n_data = mesh.shape["data"]
    batch_spec = P(("replica", "data"))

    def local_step(hidden_in, grad_out, gain_attn, gain_mlp, w_qkv, w_out, w_up, w_down):
        layers, width = gain_attn.shape
        matrix_units = (w_qkv[0].size + w_out[0].size + w_up[0].size + w_down[0].size) // 2048
        share_units = matrix_units // n_data
        chunk_units = share_units // CHUNKS + 1
        total_units = matrix_units + CHUNKS
        window_rows = 16 * chunk_units * CHUNKS
        gain_rows = 2 * width // 128
        share = (matrix_units * 2048 + 2 * width) // n_data

        act_in = hidden_in
        back_fns = []
        for layer in range(layers):
            act_in, back_fn = block_forward(act_in, gain_attn[layer], gain_mlp[layer], w_qkv[layer], w_out[layer], w_up[layer], w_down[layer], total_units)
            back_fns.append(back_fn)
        order = Order()

        def make_segments(layer, grad_act):
            return back_fns[layer](grad_out if grad_act is None else grad_act, order)

        def make_chunk(flat, chunk_idx):
            return Chunk(order, flat, chunk_idx, chunk_units, share_units, total_dev)

        windows = jnp.zeros((layers, chunk_units * CHUNKS, 16, 128), jnp.float32)
        grad_act, windows = run_plan(layers, make_segments, make_chunk, windows, order)
        windows = windows.reshape(layers, window_rows, 128)
        tail = 16 * CHUNKS
        blk = tail * -(-(share // 128 + 1) // (16 * tail))
        grads = place_output(windows, share, blk, tail, tail - gain_rows, 2 * gain_rows // n_data)
        return grad_act, grads

    return jax.shard_map(local_step, mesh=mesh, in_specs=(batch_spec, batch_spec, P(), P(), P(), P(), P(), P()), out_specs=(batch_spec, P(None, "data")), check_vma=False)
```
